512 devices in a mesh: ep: 64 (over z, y_hi, core), edp: 8 (over y_lo, x).
Axes of the slice: x: 4, y: 8 (y_hi: 4, y_lo: 2; y = y_hi * 2 + y_lo), z: 8, core: 2. Of those that a mesh axis runs over, the one named last changes fastest.
Arguments:
- expert_grads: bfloat16 [64, 8, 32, 7168], P('ep', 'edp'), may hold values from -1.59375 to 1.59375
- expert_param: float32 [64, 32, 7168], P('ep', 'edp'), may hold values from -3 to 3
- expert_moment: float32 [64, 32, 7168], P('ep', 'edp'), may hold values from -1.2 to 1.2
- expert_second: float32 [64, 32, 7168], P('ep', 'edp'), may hold values from 0.01 to 1
- dense_grads: bfloat16 [64, 8, 64, 7168], P('ep', 'edp'), may hold values from -1.59375 to 1.59375
- dense_param: float32 [458752], P(('ep', 'edp')), may hold values from -3 to 3
- dense_moment: float32 [458752], P(('ep', 'edp')), may hold values from -1.2 to 1.2
- dense_second: float32 [458752], P(('ep', 'edp')), may hold values from 0.01 to 1
- writer: int32 [64, 8, 1], P('ep', 'edp'), may hold values from 0 to 7; in each aligned block of 8 rows (0 to 7, 8 to 15, ..., all dimensions but the last counted through in order) at most 4 rows name the same one
- live_blocks: int32 [64, 8], P('ep', 'edp'), may hold values from 1 to 224
Outputs:
- expert_param_out: float32 [64, 32, 7168], P('ep', 'edp')
- expert_moment_out: float32 [64, 32, 7168], P('ep', 'edp')
- expert_second_out: float32 [64, 32, 7168], P('ep', 'edp')
- dense_param_out: float32 [458752], P(('ep', 'edp'))
- dense_moment_out: float32 [458752], P(('ep', 'edp'))
- dense_second_out: float32 [458752], P(('ep', 'edp'))
- save_slots: bfloat16 [64, 8, 4, 28672], P('ep', 'edp')
The draws below stay inside these ranges and needn't reach their ends.
Inputs may be any that keep to these rules, and one draw needn't show every extreme that they name: `writer`: within one expert no rank stores more than 4 slices, and in some experts one rank stores exactly 4.
All inputs are finite; a program needn't handle non-finite values.
Results may differ from the reference program's by a relative error of at most 0.013.
Values may be sent and summed in bfloat16 or wider, within the bound.
No kernel may reach another device: no remote copies, remote signals or barrier semaphores. Data moves between devices by JAX's collectives and lax.ppermute only.
A program may use at most 64 MiB of HBM per device.

```python
import math
import jax
import jax.numpy as jnp
import numpy as np
from jax import lax

D = 7168
SR = 4
DR = 64
EXPERTS = 64
R = 32
BLK = 224
MOST = 4
DFLAT = 458752
N_EP = 64
N_EDP = 8


def plant(drawn, rng, smallest, largest):
    shape = drawn.shape
    spot = [jax.random.randint(jax.random.fold_in(rng, axis), (), 0, shape[axis]) for axis in range(len(shape))]
    drawn = drawn.at[tuple(spot)].set(smallest)
    longest = shape.index(max(shape))
    spot[longest] = (spot[longest] + 1) % shape[longest]
    return drawn.at[tuple(spot)].set(largest)


def raised(entries, stream_key, source, target, shards_of, factor):
    owner, partner = [(jnp.arange(entries.shape[axis_at]) // (entries.shape[axis_at] // shards_of)).reshape([-1 if axis == axis_at else 1 for axis in range(entries.ndim)]) for axis_at in (source, target)]
    chosen = jax.random.permutation(stream_key, shards_of)[partner]
    strong = (owner == chosen) | (owner == (partner + shards_of // 2) % shards_of)
    return jnp.where(strong, factor * entries, entries)


def steps_of(rng, shape, split, low, high):
    gain = 1.0
    for dim, blocks in split:
        steps = jax.random.uniform(jax.random.fold_in(jax.random.fold_in(rng, 6), dim), (blocks,), jnp.float32, low / len(split), high / len(split))
        gain = gain * jnp.repeat(jnp.exp(steps), shape[dim] // blocks).reshape((-1,) + (1,) * (len(shape) - 1 - dim))
    return gain


def assign_block(key, own, number, rows, number_of, top, limit, lean):
    ranking = jax.random.permutation(key, number_of)
    crowded, common = load_shares(number_of, rows * top, limit, lean, True), load_shares(number_of, rows * top, limit, lean, False)
    places = jnp.arange(number_of)

    def named(lengths, offset_by):
        used = int((lengths > 0).sum())
        fixed = max(1, used // 4)
        passed = fixed + (places - fixed + offset_by * (used - fixed)) % max(1, number_of - fixed)
        return jnp.zeros((number_of,), jnp.int32).at[ranking[jnp.where(places < fixed, places, passed)]].set(jnp.asarray(lengths, jnp.int32))

    lengths = jnp.where(number % 4 == 0, named(crowded, number // 4), named(common, number - number // 4 - 1))
    mixed = jax.random.permutation(jax.random.fold_in(own, 3), number_of)
    donor, receiver = mixed[0:number_of // 2 * 2:2], mixed[1:number_of // 2 * 2:2]
    margin = jnp.minimum(lengths[donor] - 1, limit - lengths[receiver]) // 2
    margin = jnp.where((donor == ranking[0]) | (receiver == ranking[0]) | (lengths[receiver] == 0), 0, jnp.maximum(margin, 0))
    passed = jax.random.randint(jax.random.fold_in(own, 4), (number_of // 2,), 0, 1 << 20) % (margin + 1)
    lengths = lengths.at[donor].add(-passed).at[receiver].add(passed)
    items = jnp.searchsorted(jnp.cumsum(lengths), jnp.arange(rows * top), side="right").astype(jnp.int32)
    table = items.reshape(top, rows).T
    table = table[jax.random.permutation(jax.random.fold_in(own, 1), rows)]
    offset_by = jax.random.randint(jax.random.fold_in(own, 2), (rows, 1), 0, top)
    return jnp.take_along_axis(table, (jnp.arange(top)[None, :] + offset_by) % top, axis=1)


def load_shares(count, total, reach, slope, full):
    loads = [(1 << 20) // math.isqrt(grade ** slope) + 1 for grade in range(1, count + 1)]
    largest = reach if full else min(reach, max(-(-total // count), total * loads[0] // sum(loads)))
    least = 1 if total - largest >= count - 1 else 0
    holding, rest = [largest] + [least] * (count - 1), total - largest - least * (count - 1)
    while rest > 0:
        candidates = [i for i in range(1, count) if holding[i] < largest] or [i for i in range(1, count) if holding[i] < reach]
        mass, budget = sum([loads[i] for i in candidates]), rest
        for i in candidates:
            more = min(reach - holding[i], max(1, budget * loads[i] // mass), rest)
            holding[i] = holding[i] + more
            rest = rest - more
    return np.array(holding)


def normal_values(key, dims, scale, limit, shards=(), held_as=jnp.bfloat16):
    array = scale * jax.random.normal(key, dims, jnp.float32)
    if shards:
        array = array * steps_of(key, dims, shards, -0.22, 0.18)
    return jnp.clip(array, -limit, limit).astype(held_as)


def heavy_noise(key, shape, spread, most, split, heavy, kind=jnp.bfloat16):
    result = spread * jax.random.normal(key, shape, jnp.float32)
    if split:
        result = result * steps_of(key, shape, split, -0.22, 0.18)
    return jnp.clip(raised(result, jax.random.fold_in(key, 3), *heavy), -most, most).astype(kind)


def setup_inputs(seed: int = 0) -> dict:
    streams_of = jax.random.split(jax.random.key(seed), 11)
    expert_grads = heavy_noise(streams_of[0], (EXPERTS, N_EDP, R, D), 0.2, 1.59375, ((0, 64), (1, 8)), (1, 2, 8, 2.0))
    expert_param = normal_values(streams_of[1], (EXPERTS, R, D), 0.5, 3.0, ((0, 64), (1, 8)), jnp.float32)
    expert_moment = normal_values(streams_of[2], (EXPERTS, R, D), 0.2, 1.2, ((0, 64), (1, 8)), jnp.float32)
    expert_second = jnp.clip(jnp.exp(math.log(1.0) - 4.6051702 * jax.random.uniform(streams_of[3], (EXPERTS, R, D), jnp.float32) ** steps_of(streams_of[3], (EXPERTS, R, D), ((0, 64), (1, 8)), -0.2, 0.2)), 0.01, 1.0)
    dense_grads = normal_values(streams_of[4], (N_EP, N_EDP, DR, D), 0.2, 1.59375, ((0, 64), (1, 8)))
    dense_param = normal_values(streams_of[5], (DFLAT,), 0.5, 3.0, ((0, 512),), jnp.float32)
    dense_moment = normal_values(streams_of[6], (DFLAT,), 0.2, 1.2, ((0, 512),), jnp.float32)
    dense_second = jnp.clip(jnp.exp(math.log(1.0) - 4.6051702 * jax.random.uniform(streams_of[7], (DFLAT,), jnp.float32) ** steps_of(streams_of[7], (DFLAT,), ((0, 512),), -0.2, 0.2)), 0.01, 1.0)
    writer_keys = jax.random.split(jax.random.fold_in(streams_of[8], 1), EXPERTS * N_EDP // N_EDP)
    writer_turns = jax.random.permutation(jax.random.fold_in(streams_of[8], 3), EXPERTS * N_EDP // N_EDP)
    writer = jax.vmap(lambda own, number: assign_block(jax.random.fold_in(streams_of[8], 2), own, number, N_EDP, N_EDP, 1, MOST, 2))(writer_keys, writer_turns).reshape((EXPERTS, N_EDP, 1))
    live_blocks = plant(jax.random.randint(streams_of[9], (EXPERTS, N_EDP), 1, BLK + 1), jax.random.fold_in(streams_of[9], 1), 1, BLK).astype(jnp.int32)
    return dict(expert_grads=expert_grads, expert_param=expert_param, expert_moment=expert_moment, expert_second=expert_second, dense_grads=dense_grads, dense_param=dense_param, dense_moment=dense_moment, dense_second=dense_second, writer=writer, live_blocks=live_blocks)


BETA_FIRST = 0.9
BETA_SECOND = 0.95
LEARN_RATE = 0.01
DECAY_RATE = 0.1
EPSILON = 1e-08
FIRST_BIAS = 1.0 - BETA_FIRST ** 10
SECOND_BIAS = 1.0 - BETA_SECOND ** 10

def adam_update(master, moment, second, gradient):
    moment_new = BETA_FIRST * moment + (1.0 - BETA_FIRST) * gradient
    second_new = BETA_SECOND * second + (1.0 - BETA_SECOND) * gradient * gradient
    direction = moment_new / FIRST_BIAS / (jnp.sqrt(second_new / SECOND_BIAS) + EPSILON)
    master_new = master - LEARN_RATE * (direction + DECAY_RATE * master)
    return (master_new, moment_new, second_new)

def reference(expert_grads, expert_param, expert_moment, expert_second, dense_grads, dense_param, dense_moment, dense_second, writer, live_blocks):
    expert_sum = lax.optimization_barrier(jnp.sum(expert_grads, axis=1, dtype=jnp.float32))
    expert_new, expert_mom, expert_sec = adam_update(expert_param, expert_moment, expert_second, expert_sum)
    dense_sum = lax.optimization_barrier(jnp.sum(dense_grads, axis=(0, 1), dtype=jnp.float32)).reshape(-1)
    dense_new, dense_mom, dense_sec = adam_update(dense_param, dense_moment, dense_second, dense_sum)
    rounded = lax.optimization_barrier(expert_new.astype(jnp.bfloat16))
    slices = rounded.astype(jnp.float32).reshape(EXPERTS, N_EDP, SR * D)
    positions = jnp.arange(SR * D, dtype=jnp.int32) // 128
    kept_slices = jnp.where(positions[None, None, :] < live_blocks[:, :, None], slices, jnp.zeros_like(slices))
    writer_ids = writer[:, :, 0]
    same_writer = writer_ids[:, :, None] == writer_ids[:, None, :]
    earlier = lax.broadcasted_iota(jnp.int32, (N_EDP, N_EDP), 1) < lax.broadcasted_iota(jnp.int32, (N_EDP, N_EDP), 0)
    slot_rank = lax.optimization_barrier(jnp.sum((same_writer & earlier[None]).astype(jnp.int32), axis=2))
    owners = jnp.arange(N_EDP, dtype=jnp.int32)
    slot_ids = jnp.arange(MOST, dtype=jnp.int32)
    selector = (writer_ids[:, None, None, :] == owners[None, :, None, None]) & (slot_rank[:, None, None, :] == slot_ids[None, None, :, None])
    saved_slots = jnp.einsum('ewkr,erx->ewkx', selector.astype(jnp.float32), kept_slices).astype(jnp.bfloat16)
    return (expert_new, expert_mom, expert_sec, dense_new, dense_mom, dense_sec, saved_slots)
```

```python
import jax
import jax.numpy as jnp
from jax import lax
from jax.sharding import Mesh, PartitionSpec as P

BETA_FIRST = 0.9
BETA_SECOND = 0.95
LEARN_RATE = 0.01
DECAY_RATE = 0.1
EPSILON = 1e-08
FIRST_BIAS = 1.0 - BETA_FIRST**10
SECOND_BIAS = 1.0 - BETA_SECOND**10
EP = ("z", "yh", "c")
EDP = ("yl", "x")
ABSENT = 2.0**100


def adam_update(master, moment, second, gradient):
    moment_new = BETA_FIRST * moment + (1.0 - BETA_FIRST) * gradient
    second_new = BETA_SECOND * second + (1.0 - BETA_SECOND) * gradient * gradient
    direction = moment_new / FIRST_BIAS / (jnp.sqrt(second_new / SECOND_BIAS) + EPSILON)
    master_new = master - LEARN_RATE * (direction + DECAY_RATE * master)
    return (master_new, moment_new, second_new)


def to_tiles(x):
    return x.reshape(4, 56, 128).transpose(1, 0, 2).reshape(224, 128)


def from_tiles(x):
    return x.reshape(56, 4, 128).transpose(1, 0, 2).reshape(4, 7168)


def body(
    expert_grads,
    expert_param,
    expert_moment,
    expert_second,
    dense_grads,
    dense_param,
    dense_moment,
    dense_second,
    writer,
    live_blocks,
):
    expert_part = expert_grads[0, 0].reshape(8, 4, 56, 128).transpose(0, 2, 1, 3)
    expert_part = expert_part.reshape(8, 224, 128)
    dense_part = dense_grads[0, 0].reshape(8, 8, 8, 7, 128).transpose(2, 0, 3, 1, 4)
    dense_part = dense_part.reshape(8, 448, 128)
    outgoing = jnp.concatenate([expert_part, dense_part], axis=1)
    arrived = lax.all_to_all(outgoing, EDP, split_axis=0, concat_axis=0, tiled=True)
    expert_sum = arrived[:, :224].astype(jnp.float32).sum(axis=0)
    dense_partial = arrived[:, 224:].astype(jnp.float32).sum(axis=0)

    expert_new, expert_mom, expert_sec = adam_update(
        to_tiles(expert_param[0]), to_tiles(expert_moment[0]), to_tiles(expert_second[0]), expert_sum
    )
    row = lax.broadcasted_iota(jnp.int32, (224, 128), 0)
    block = (row % 4) * 56 + row // 4
    kept = jnp.where(block < live_blocks[0, 0], expert_new, 0.0).astype(jnp.bfloat16)
    rank = lax.broadcasted_iota(jnp.int32, (8, 224, 128), 0)
    slices = jnp.where(rank == writer[0, 0, 0], kept[None], jnp.bfloat16(ABSENT))
    received = lax.all_to_all(slices, EDP, split_axis=0, concat_axis=0, tiled=True)

    core = lax.axis_index("c")
    rows = dense_partial.reshape(8, 7, 8, 128).transpose(0, 2, 1, 3).reshape(32, 2, 7, 128)
    mine = jnp.where(core == 0, rows[:, 0], rows[:, 1])
    other = jnp.where(core == 0, rows[:, 1], rows[:, 0])
    swapped = lax.ppermute(other, "c", [(0, 1), (1, 0)])
    pair = jnp.pad(mine + swapped, ((0, 0), (0, 1), (0, 0)))
    dense_arrived = lax.all_to_all(pair, ("z", "yh"), split_axis=0, concat_axis=0, tiled=True)
    dense_sum = dense_arrived.sum(axis=0)[:7].reshape(-1)

    present = (received[:, 0, 0].astype(jnp.float32) < ABSENT / 2)
    index = lax.broadcasted_iota(jnp.int32, (8, 8), 0)
    index2 = lax.broadcasted_iota(jnp.int32, (8, 8), 1)
    before = jnp.sum(jnp.where((index2 < index) & present[None, :], 1, 0), axis=1)
    slot = lax.broadcasted_iota(jnp.int32, (4, 8), 0)
    selector = ((slot == before[None, :]) & present[None, :]).astype(jnp.bfloat16)
    clean = jnp.where(present[:, None, None], received, jnp.bfloat16(0))
    saved = jnp.einsum("kr,rql->kql", selector, clean, preferred_element_type=jnp.float32)
    saved = saved.astype(jnp.bfloat16).reshape(4, 56, 4, 128).transpose(0, 2, 1, 3).reshape(4, 28672)

    dense_new, dense_mom, dense_sec = adam_update(
        dense_param, dense_moment, dense_second, dense_sum
    )
    return (
        from_tiles(expert_new)[None],
        from_tiles(expert_mom)[None],
        from_tiles(expert_sec)[None],
        dense_new,
        dense_mom,
        dense_sec,
        saved[None, None],
    )


def solution(mesh):
    fine = Mesh(mesh.devices.reshape(8, 4, 2, 2, 4), EP + EDP)
    state = P(EP, EDP, None)
    flat = P(EP + EDP)
    return jax.shard_map(
        body,
        mesh=fine,
        in_specs=(
            P(EP, EDP, None, None),
            state,
            state,
            state,
            P(EP, EDP, None, None),
            flat,
            flat,
            flat,
            state,
            P(EP, EDP),
        ),
        out_specs=(state, state, state, flat, flat, flat, P(EP, EDP, None, None)),
        check_vma=False,
    )
```

```python
import jax
import jax.numpy as jnp
from jax import lax
from jax.sharding import Mesh, PartitionSpec as P


BETA_FIRST = 0.9
BETA_SECOND = 0.95
LEARN_RATE = 0.01
DECAY_RATE = 0.1
EPSILON = 1e-08
FIRST_BIAS = 1.0 - BETA_FIRST**10
SECOND_BIAS = 1.0 - BETA_SECOND**10
EP = ("z", "yh", "c")
EDP = ("yl", "x")
ABSENT = 2.0**100


def adam_update(master, moment, second, gradient):
    moment_new = BETA_FIRST * moment + (1.0 - BETA_FIRST) * gradient
    second_new = BETA_SECOND * second + (1.0 - BETA_SECOND) * gradient * gradient
    direction = moment_new / FIRST_BIAS / (jnp.sqrt(second_new / SECOND_BIAS) + EPSILON)
    master_new = master - LEARN_RATE * (direction + DECAY_RATE * master)
    return (master_new, moment_new, second_new)


def to_tiles(x):
    return x.reshape(4, 56, 128).transpose(1, 0, 2).reshape(224, 128)


def from_tiles(x):
    return x.reshape(56, 4, 128).transpose(1, 0, 2).reshape(4, 7168)


def body(
    expert_grads,
    expert_param,
    expert_moment,
    expert_second,
    dense_grads,
    dense_param,
    dense_moment,
    dense_second,
    writer,
    live_blocks,
):
    outgoing = expert_grads[0, 0].reshape(8, 4, 7168)
    arrived = lax.all_to_all(outgoing, EDP, split_axis=0, concat_axis=0, tiled=True)
    expert_sum = to_tiles(arrived.astype(jnp.float32).sum(axis=0))

    core = lax.axis_index("c")
    out_row = lax.broadcasted_iota(jnp.int32, (64, 64), 0)
    in_row = lax.broadcasted_iota(jnp.int32, (64, 64), 1)
    wanted = 2 * (out_row % 32) + jnp.where(out_row < 32, core, 1 - core)
    parting = (in_row == wanted).astype(jnp.bfloat16)
    parted = jnp.dot(parting, dense_grads[0, 0], preferred_element_type=jnp.float32)
    parted = parted.astype(jnp.bfloat16)
    swapped = lax.ppermute(parted[32:], "c", [(0, 1), (1, 0)])
    pair = parted[:32].astype(jnp.float32) + swapped.astype(jnp.float32)
    pair = pair.astype(jnp.bfloat16).reshape(4, 8, 8, 7, 128).transpose(2, 0, 3, 1, 4)
    pair = pair.reshape(8, 224, 128)

    expert_new, expert_mom, expert_sec = adam_update(
        to_tiles(expert_param[0]), to_tiles(expert_moment[0]), to_tiles(expert_second[0]), expert_sum
    )
    row = lax.broadcasted_iota(jnp.int32, (224, 128), 0)
    block = (row % 4) * 56 + row // 4
    kept = jnp.where(block < live_blocks[0, 0], expert_new, 0.0).astype(jnp.bfloat16)
    rank = lax.broadcasted_iota(jnp.int32, (8, 224, 128), 0)
    slices = jnp.where(rank == writer[0, 0, 0], kept[None], jnp.bfloat16(ABSENT))

    second = jnp.concatenate([slices, pair], axis=1)
    both = lax.all_to_all(second, EDP, split_axis=0, concat_axis=0, tiled=True)
    received = both[:, :224]
    partial = both[:, 224:].astype(jnp.float32).sum(axis=0)

    rows = partial.reshape(4, 7, 8, 128).transpose(0, 2, 1, 3).reshape(32, 7, 128)
    rows = jnp.pad(rows, ((0, 0), (0, 1), (0, 0)))
    dense_arrived = lax.all_to_all(rows, ("z", "yh"), split_axis=0, concat_axis=0, tiled=True)
    dense_sum = dense_arrived.sum(axis=0)[:7].reshape(-1)

    present = (received[:, 0, 0].astype(jnp.float32) < ABSENT / 2)
    index = lax.broadcasted_iota(jnp.int32, (8, 8), 0)
    index2 = lax.broadcasted_iota(jnp.int32, (8, 8), 1)
    before = jnp.sum(jnp.where((index2 < index) & present[None, :], 1, 0), axis=1)
    slot = lax.broadcasted_iota(jnp.int32, (4, 8), 0)
    selector = ((slot == before[None, :]) & present[None, :]).astype(jnp.bfloat16)
    clean = jnp.where(present[:, None, None], received, jnp.bfloat16(0))
    saved = jnp.einsum("kr,rql->kql", selector, clean, preferred_element_type=jnp.float32)
    saved = saved.astype(jnp.bfloat16).reshape(4, 56, 4, 128).transpose(0, 2, 1, 3).reshape(4, 28672)

    dense_new, dense_mom, dense_sec = adam_update(
        dense_param, dense_moment, dense_second, dense_sum
    )
    return (
        from_tiles(expert_new)[None],
        from_tiles(expert_mom)[None],
        from_tiles(expert_sec)[None],
        dense_new,
        dense_mom,
        dense_sec,
        saved[None, None],
    )


def solution(mesh):
    fine = Mesh(mesh.devices.reshape(8, 4, 2, 2, 4), EP + EDP)
    state = P(EP, EDP, None)
    flat = P(EP + EDP)
    return jax.shard_map(
        body,
        mesh=fine,
        in_specs=(
            P(EP, EDP, None, None),
            state,
            state,
            state,
            P(EP, EDP, None, None),
            flat,
            flat,
            flat,
            state,
            P(EP, EDP),
        ),
        out_specs=(state, state, state, flat, flat, flat, P(EP, EDP, None, None)),
        check_vma=False,
    )
```

```python
import jax
import jax.numpy as jnp
from jax import lax
from jax.sharding import Mesh, PartitionSpec as P


BETA_FIRST = 0.9
BETA_SECOND = 0.95
LEARN_RATE = 0.01
DECAY_RATE = 0.1
EPSILON = 1e-08
FIRST_BIAS = 1.0 - BETA_FIRST**10
SECOND_BIAS = 1.0 - BETA_SECOND**10
EP = ("z", "yh", "c")
EDP = ("yl", "x")
ABSENT = 2.0**100


def adam_update(master, moment, second, gradient):
    moment_new = BETA_FIRST * moment + (1.0 - BETA_FIRST) * gradient
    second_new = BETA_SECOND * second + (1.0 - BETA_SECOND) * gradient * gradient
    direction = moment_new / FIRST_BIAS / (jnp.sqrt(second_new / SECOND_BIAS) + EPSILON)
    master_new = master - LEARN_RATE * (direction + DECAY_RATE * master)
    return (master_new, moment_new, second_new)


def to_tiles(x):
    return x.reshape(4, 56, 128).transpose(1, 0, 2).reshape(224, 128)


def from_tiles(x):
    return x.reshape(56, 4, 128).transpose(1, 0, 2).reshape(4, 7168)


def body(
    expert_grads,
    expert_param,
    expert_moment,
    expert_second,
    dense_grads,
    dense_param,
    dense_moment,
    dense_second,
    writer,
    live_blocks,
):
    outgoing = expert_grads[0, 0].reshape(8, 4, 7168)
    arrived = lax.all_to_all(outgoing, EDP, split_axis=0, concat_axis=0, tiled=True)
    expert_sum = to_tiles(arrived.astype(jnp.float32).sum(axis=0))
    state = (to_tiles(expert_param[0]), to_tiles(expert_moment[0]), to_tiles(expert_second[0]))

    core = lax.axis_index("c")
    out_row = lax.broadcasted_iota(jnp.int32, (64, 64), 0)
    in_row = lax.broadcasted_iota(jnp.int32, (64, 64), 1)
    wanted = 2 * (out_row % 32) + jnp.where(out_row < 32, core, 1 - core)
    parting = (in_row == wanted).astype(jnp.bfloat16)
    parted = jnp.dot(parting, dense_grads[0, 0], preferred_element_type=jnp.float32)
    parted = parted.astype(jnp.bfloat16)
    swapped = lax.ppermute(parted[32:], "c", [(0, 1), (1, 0)])
    pair = parted[:32].astype(jnp.float32) + swapped.astype(jnp.float32)
    pair = pair.astype(jnp.bfloat16).reshape(4, 8, 8, 7, 128).transpose(2, 0, 3, 1, 4)
    pair = pair.reshape(8, 224, 128)

    expert_new, _, _ = adam_update(*state, expert_sum)
    row = lax.broadcasted_iota(jnp.int32, (224, 128), 0)
    block = (row % 4) * 56 + row // 4
    kept = jnp.where(block < live_blocks[0, 0], expert_new, 0.0).astype(jnp.bfloat16)
    rank = lax.broadcasted_iota(jnp.int32, (8, 224, 128), 0)
    slices = jnp.where(rank == writer[0, 0, 0], kept[None], jnp.bfloat16(ABSENT))

    second = jnp.concatenate([slices, pair], axis=1)
    both = lax.all_to_all(second, EDP, split_axis=0, concat_axis=0, tiled=True)
    partial = both[:, 224:].astype(jnp.float32).sum(axis=0)

    rows = partial.reshape(4, 7, 8, 128).transpose(0, 2, 1, 3).reshape(32, 7, 128)
    rows = rows.astype(jnp.bfloat16)
    last = lax.all_to_all(rows, ("z", "yh"), split_axis=0, concat_axis=0, tiled=True)
    dense_sum = last.astype(jnp.float32).sum(axis=0).reshape(-1)

    state, expert_sum, both, _ = lax.optimization_barrier((state, expert_sum, both, rows))
    received = both[:, :224]
    expert_new, expert_mom, expert_sec = adam_update(*state, expert_sum)
    expert_new, expert_mom, expert_sec = (
        from_tiles(expert_new),
        from_tiles(expert_mom),
        from_tiles(expert_sec),
    )

    present = (received[:, 0, 0].astype(jnp.float32) < ABSENT / 2)
    index = lax.broadcasted_iota(jnp.int32, (8, 8), 0)
    index2 = lax.broadcasted_iota(jnp.int32, (8, 8), 1)
    before = jnp.sum(jnp.where((index2 < index) & present[None, :], 1, 0), axis=1)
    slot = lax.broadcasted_iota(jnp.int32, (4, 8), 0)
    selector = ((slot == before[None, :]) & present[None, :]).astype(jnp.bfloat16)
    clean = jnp.where(present[:, None, None], received, jnp.bfloat16(0))
    saved = jnp.einsum("kr,rql->kql", selector, clean, preferred_element_type=jnp.float32)
    saved = saved.astype(jnp.bfloat16).reshape(4, 56, 4, 128)
    saved = saved.transpose(0, 2, 1, 3).reshape(4, 28672)

    dense_new, dense_mom, dense_sec = adam_update(
        dense_param, dense_moment, dense_second, dense_sum
    )
    return (
        expert_new[None],
        expert_mom[None],
        expert_sec[None],
        dense_new,
        dense_mom,
        dense_sec,
        saved[None, None],
    )


def solution(mesh):
    fine = Mesh(mesh.devices.reshape(8, 4, 2, 2, 4), EP + EDP)
    state = P(EP, EDP, None)
    flat = P(EP + EDP)
    return jax.shard_map(
        body,
        mesh=fine,
        in_specs=(
            P(EP, EDP, None, None),
            state,
            state,
            state,
            P(EP, EDP, None, None),
            flat,
            flat,
            flat,
            state,
            P(EP, EDP),
        ),
        out_specs=(state, state, state, flat, flat, flat, P(EP, EDP, None, None)),
        check_vma=False,
    )
```

```python
import jax
import jax.numpy as jnp
from jax import lax
from jax.sharding import Mesh, PartitionSpec as P


BETA_FIRST = 0.9
BETA_SECOND = 0.95
LEARN_RATE = 0.01
DECAY_RATE = 0.1
EPSILON = 1e-08
FIRST_BIAS = 1.0 - BETA_FIRST**10
SECOND_BIAS = 1.0 - BETA_SECOND**10
EP = ("zy", "c")
EDP = "r"
FIRST = 30
MEMBERS = [(FIRST + j) % 32 for j in range(32)]
ABSENT = 2.0**100


def adam_update(master, moment, second, gradient):
    moment_new = BETA_FIRST * moment + (1.0 - BETA_FIRST) * gradient
    second_new = BETA_SECOND * second + (1.0 - BETA_SECOND) * gradient * gradient
    direction = moment_new / FIRST_BIAS / (jnp.sqrt(second_new / SECOND_BIAS) + EPSILON)
    master_new = master - LEARN_RATE * (direction + DECAY_RATE * master)
    return (master_new, moment_new, second_new)


def to_tiles(x):
    return x.reshape(4, 56, 128).transpose(1, 0, 2).reshape(224, 128)


def from_tiles(x):
    return x.reshape(56, 4, 128).transpose(1, 0, 2).reshape(4, 7168)


def body(
    expert_grads,
    expert_param,
    expert_moment,
    expert_second,
    dense_grads,
    dense_param,
    dense_moment,
    dense_second,
    writer,
    live_blocks,
):
    outgoing = expert_grads[0, 0].reshape(8, 4, 7168)
    arrived = lax.all_to_all(outgoing, EDP, split_axis=0, concat_axis=0, tiled=True)
    expert_sum = to_tiles(arrived.astype(jnp.float32).sum(axis=0))
    state = (to_tiles(expert_param[0]), to_tiles(expert_moment[0]), to_tiles(expert_second[0]))

    core = lax.axis_index("c")
    out_row = lax.broadcasted_iota(jnp.int32, (64, 64), 0)
    in_row = lax.broadcasted_iota(jnp.int32, (64, 64), 1)
    wanted = 2 * (out_row % 32) + jnp.where(out_row < 32, core, 1 - core)
    parting = (in_row == wanted).astype(jnp.bfloat16)
    parted = jnp.dot(parting, dense_grads[0, 0], preferred_element_type=jnp.float32)
    parted = parted.astype(jnp.bfloat16)
    swapped = lax.ppermute(parted[32:], "c", [(0, 1), (1, 0)])
    pair = parted[:32].astype(jnp.float32) + swapped.astype(jnp.float32)
    pair = pair.astype(jnp.bfloat16).reshape(4, 8, 8, 7, 128).transpose(2, 0, 3, 1, 4)
    pair = pair.reshape(8, 224, 128)

    expert_new, _, _ = adam_update(*state, expert_sum)
    row = lax.broadcasted_iota(jnp.int32, (224, 128), 0)
    block = (row % 4) * 56 + row // 4
    kept = jnp.where(block < live_blocks[0, 0], expert_new, 0.0).astype(jnp.bfloat16)
    rank = lax.broadcasted_iota(jnp.int32, (8, 224, 128), 0)
    slices = jnp.where(rank == writer[0, 0, 0], kept[None], jnp.bfloat16(ABSENT))

    second = jnp.concatenate([slices, pair], axis=1)
    both = lax.all_to_all(second, EDP, split_axis=0, concat_axis=0, tiled=True)
    partial = both[:, 224:].astype(jnp.float32).sum(axis=0)

    rows = partial.reshape(4, 7, 8, 128).transpose(0, 2, 1, 3).reshape(32, 7, 128)
    rows = rows.astype(jnp.bfloat16)
    rows = jnp.concatenate([rows[FIRST:], rows[:FIRST]], axis=0)
    last = lax.all_to_all(
        rows, "zy", split_axis=0, concat_axis=0, tiled=True, axis_index_groups=[MEMBERS]
    )
    dense_sum = last.astype(jnp.float32).sum(axis=0).reshape(-1)

    state, expert_sum, both, _ = lax.optimization_barrier((state, expert_sum, both, rows))
    received = both[:, :224]
    expert_new, expert_mom, expert_sec = adam_update(*state, expert_sum)
    expert_new, expert_mom, expert_sec = (
        from_tiles(expert_new),
        from_tiles(expert_mom),
        from_tiles(expert_sec),
    )

    present = (received[:, 0, 0].astype(jnp.float32) < ABSENT / 2)
    index = lax.broadcasted_iota(jnp.int32, (8, 8), 0)
    index2 = lax.broadcasted_iota(jnp.int32, (8, 8), 1)
    before = jnp.sum(jnp.where((index2 < index) & present[None, :], 1, 0), axis=1)
    slot = lax.broadcasted_iota(jnp.int32, (4, 8), 0)
    selector = ((slot == before[None, :]) & present[None, :]).astype(jnp.bfloat16)
    clean = jnp.where(present[:, None, None], received, jnp.bfloat16(0))
    saved = jnp.einsum("kr,rql->kql", selector, clean, preferred_element_type=jnp.float32)
    saved = saved.astype(jnp.bfloat16).reshape(4, 56, 4, 128)
    saved = saved.transpose(0, 2, 1, 3).reshape(4, 28672)

    dense_new, dense_mom, dense_sec = adam_update(
        dense_param, dense_moment, dense_second, dense_sum
    )
    return (
        expert_new[None],
        expert_mom[None],
        expert_sec[None],
        dense_new,
        dense_mom,
        dense_sec,
        saved[None, None],
    )


def solution(mesh):
    fine = Mesh(mesh.devices.reshape(32, 2, 8), EP + (EDP,))
    state = P(EP, EDP, None)
    flat = P(EP + (EDP,))
    return jax.shard_map(
        body,
        mesh=fine,
        in_specs=(
            P(EP, EDP, None, None),
            state,
            state,
            state,
            P(EP, EDP, None, None),
            flat,
            flat,
            flat,
            state,
            P(EP, EDP),
        ),
        out_specs=(state, state, state, flat, flat, flat, P(EP, EDP, None, None)),
        check_vma=False,
    )
```

```python
import jax
import jax.numpy as jnp
from jax import lax
from jax.experimental import pallas as pl
from jax.sharding import Mesh, PartitionSpec as P


BETA_FIRST = 0.9
BETA_SECOND = 0.95
LEARN_RATE = 0.01
DECAY_RATE = 0.1
EPSILON = 1e-08
FIRST_BIAS = 1.0 - BETA_FIRST**10
SECOND_BIAS = 1.0 - BETA_SECOND**10
EP = ("zy", "c")
EDP = "r"
FIRST = 30
MEMBERS = [(FIRST + j) % 32 for j in range(32)]
LEAD = 2
RANKS = [(LEAD + j) % 8 for j in range(8)]
ABSENT = 2.0**100


def adam_update(master, moment, second, gradient):
    moment_new = BETA_FIRST * moment + (1.0 - BETA_FIRST) * gradient
    second_new = BETA_SECOND * second + (1.0 - BETA_SECOND) * gradient * gradient
    direction = moment_new / FIRST_BIAS / (jnp.sqrt(second_new / SECOND_BIAS) + EPSILON)
    master_new = master - LEARN_RATE * (direction + DECAY_RATE * master)
    return (master_new, moment_new, second_new)


def to_tiles(x):
    return x.reshape(4, 56, 128).transpose(1, 0, 2).reshape(224, 128)


def from_tiles(x):
    return x.reshape(56, 4, 128).transpose(1, 0, 2).reshape(4, 7168)


def chunk_kernel(rows_ref, chunks_ref):
    for place, rank in enumerate(RANKS):
        chunks_ref[place] = rows_ref[4 * rank : 4 * rank + 4, :]


def body(
    expert_grads,
    expert_param,
    expert_moment,
    expert_second,
    dense_grads,
    dense_param,
    dense_moment,
    dense_second,
    writer,
    live_blocks,
):
    outgoing = pl.pallas_call(
        chunk_kernel,
        grid=(2,),
        in_specs=[pl.BlockSpec((32, 3584), lambda half: (0, half))],
        out_specs=pl.BlockSpec((8, 4, 3584), lambda half: (0, 0, half)),
        out_shape=jax.ShapeDtypeStruct((8, 4, 7168), jnp.bfloat16),
        name="chunks",
    )(expert_grads[0, 0])
    arrived = lax.all_to_all(
        outgoing, EDP, split_axis=0, concat_axis=0, tiled=True, axis_index_groups=[RANKS]
    )
    expert_sum = to_tiles(arrived.astype(jnp.float32).sum(axis=0))
    state = (to_tiles(expert_param[0]), to_tiles(expert_moment[0]), to_tiles(expert_second[0]))

    core = lax.axis_index("c")
    out_row = lax.broadcasted_iota(jnp.int32, (64, 64), 0)
    in_row = lax.broadcasted_iota(jnp.int32, (64, 64), 1)
    wanted = 2 * (out_row % 32) + jnp.where(out_row < 32, core, 1 - core)
    parting = (in_row == wanted).astype(jnp.bfloat16)
    parted = jnp.dot(parting, dense_grads[0, 0], preferred_element_type=jnp.float32)
    parted = parted.astype(jnp.bfloat16)
    swapped = lax.ppermute(parted[32:], "c", [(0, 1), (1, 0)])
    pair = parted[:32].astype(jnp.float32) + swapped.astype(jnp.float32)
    pair = pair.astype(jnp.bfloat16).reshape(4, 8, 8, 7, 128).transpose(2, 0, 3, 1, 4)
    pair = pair.reshape(8, 224, 128)
    pair = jnp.concatenate([pair[LEAD:], pair[:LEAD]], axis=0)

    expert_new, _, _ = adam_update(*state, expert_sum)
    row = lax.broadcasted_iota(jnp.int32, (224, 128), 0)
    block = (row % 4) * 56 + row // 4
    kept = jnp.where(block < live_blocks[0, 0], expert_new, 0.0).astype(jnp.bfloat16)
    rank = lax.broadcasted_iota(jnp.int32, (8, 224, 128), 0)
    slices = jnp.where((rank + LEAD) % 8 == writer[0, 0, 0], kept[None], jnp.bfloat16(ABSENT))

    second = jnp.concatenate([slices, pair], axis=1)
    both = lax.all_to_all(
        second, EDP, split_axis=0, concat_axis=0, tiled=True, axis_index_groups=[RANKS]
    )
    partial = both[:, 224:].astype(jnp.float32).sum(axis=0)

    rows = partial.reshape(4, 7, 8, 128).transpose(0, 2, 1, 3).reshape(32, 7, 128)
    rows = rows.astype(jnp.bfloat16)
    rows = jnp.concatenate([rows[FIRST:], rows[:FIRST]], axis=0)
    last = lax.all_to_all(
        rows, "zy", split_axis=0, concat_axis=0, tiled=True, axis_index_groups=[MEMBERS]
    )
    dense_sum = last.astype(jnp.float32).sum(axis=0).reshape(-1)

    state, expert_sum, both, _ = lax.optimization_barrier((state, expert_sum, both, rows))
    received = both[:, :224]
    expert_new, expert_mom, expert_sec = adam_update(*state, expert_sum)
    expert_new, expert_mom, expert_sec = (
        from_tiles(expert_new),
        from_tiles(expert_mom),
        from_tiles(expert_sec),
    )

    present = (received[:, 0, 0].astype(jnp.float32) < ABSENT / 2)
    index = (lax.broadcasted_iota(jnp.int32, (8, 8), 0) + LEAD) % 8
    index2 = (lax.broadcasted_iota(jnp.int32, (8, 8), 1) + LEAD) % 8
    before = jnp.sum(jnp.where((index2 < index) & present[None, :], 1, 0), axis=1)
    slot = lax.broadcasted_iota(jnp.int32, (4, 8), 0)
    selector = ((slot == before[None, :]) & present[None, :]).astype(jnp.bfloat16)
    clean = jnp.where(present[:, None, None], received, jnp.bfloat16(0))
    saved = jnp.einsum("kr,rql->kql", selector, clean, preferred_element_type=jnp.float32)
    saved = saved.astype(jnp.bfloat16).reshape(4, 56, 4, 128)
    saved = saved.transpose(0, 2, 1, 3).reshape(4, 28672)

    dense_new, dense_mom, dense_sec = adam_update(
        dense_param, dense_moment, dense_second, dense_sum
    )
    return (
        expert_new[None],
        expert_mom[None],
        expert_sec[None],
        dense_new,
        dense_mom,
        dense_sec,
        saved[None, None],
    )


def solution(mesh):
    fine = Mesh(mesh.devices.reshape(32, 2, 8), EP + (EDP,))
    state = P(EP, EDP, None)
    flat = P(EP + (EDP,))
    return jax.shard_map(
        body,
        mesh=fine,
        in_specs=(
            P(EP, EDP, None, None),
            state,
            state,
            state,
            P(EP, EDP, None, None),
            flat,
            flat,
            flat,
            state,
            P(EP, EDP),
        ),
        out_specs=(state, state, state, flat, flat, flat, P(EP, EDP, None, None)),
        check_vma=False,
    )
```

```python
import jax
import jax.numpy as jnp
from jax import lax
from jax.experimental import pallas as pl
from jax.sharding import Mesh, PartitionSpec as P


BETA_FIRST = 0.9
BETA_SECOND = 0.95
LEARN_RATE = 0.01
DECAY_RATE = 0.1
EPSILON = 1e-08
FIRST_BIAS = 1.0 - BETA_FIRST**10
SECOND_BIAS = 1.0 - BETA_SECOND**10
EP = ("zy", "c")
EDP = "r"
FIRST = 30
MEMBERS = [(FIRST + j) % 32 for j in range(32)]
LEAD = 2
RANKS = [j % 2 * 4 + (LEAD + j // 2) % 4 for j in range(8)]
ABSENT = 2.0**100


def adam_update(master, moment, second, gradient):
    moment_new = BETA_FIRST * moment + (1.0 - BETA_FIRST) * gradient
    second_new = BETA_SECOND * second + (1.0 - BETA_SECOND) * gradient * gradient
    direction = moment_new / FIRST_BIAS / (jnp.sqrt(second_new / SECOND_BIAS) + EPSILON)
    master_new = master - LEARN_RATE * (direction + DECAY_RATE * master)
    return (master_new, moment_new, second_new)


def to_tiles(x):
    return x.reshape(4, 56, 128).transpose(1, 0, 2).reshape(224, 128)


def from_tiles(x):
    return x.reshape(56, 4, 128).transpose(1, 0, 2).reshape(4, 7168)


def rank_at(place):
    return place % 2 * 4 + (LEAD + place // 2) % 4


def chunk_kernel(rows_ref, chunks_ref):
    for place, rank in enumerate(RANKS):
        chunks_ref[place] = rows_ref[4 * rank : 4 * rank + 4, :]


def body(
    expert_grads,
    expert_param,
    expert_moment,
    expert_second,
    dense_grads,
    dense_param,
    dense_moment,
    dense_second,
    writer,
    live_blocks,
):
    outgoing = pl.pallas_call(
        chunk_kernel,
        grid=(2,),
        in_specs=[pl.BlockSpec((32, 3584), lambda half: (0, half))],
        out_specs=pl.BlockSpec((8, 4, 3584), lambda half: (0, 0, half)),
        out_shape=jax.ShapeDtypeStruct((8, 4, 7168), jnp.bfloat16),
        name="chunks",
    )(expert_grads[0, 0])
    arrived = lax.all_to_all(
        outgoing, EDP, split_axis=0, concat_axis=0, tiled=True, axis_index_groups=[RANKS]
    )
    expert_sum = to_tiles(arrived.astype(jnp.float32).sum(axis=0))
    state = (to_tiles(expert_param[0]), to_tiles(expert_moment[0]), to_tiles(expert_second[0]))

    core = lax.axis_index("c")
    out_row = lax.broadcasted_iota(jnp.int32, (64, 64), 0)
    in_row = lax.broadcasted_iota(jnp.int32, (64, 64), 1)
    wanted = 2 * (out_row % 32) + jnp.where(out_row < 32, core, 1 - core)
    parting = (in_row == wanted).astype(jnp.bfloat16)
    parted = jnp.dot(parting, dense_grads[0, 0], preferred_element_type=jnp.float32)
    parted = parted.astype(jnp.bfloat16)
    swapped = lax.ppermute(parted[32:], "c", [(0, 1), (1, 0)])
    pair = parted[:32].astype(jnp.float32) + swapped.astype(jnp.float32)
    pair = pair.astype(jnp.bfloat16).reshape(4, 8, 2, 4, 7, 128).transpose(3, 2, 0, 4, 1, 5)
    pair = pair.reshape(8, 224, 128)
    pair = jnp.concatenate([pair[2 * LEAD :], pair[: 2 * LEAD]], axis=0)

    expert_new, _, _ = adam_update(*state, expert_sum)
    row = lax.broadcasted_iota(jnp.int32, (224, 128), 0)
    block = (row % 4) * 56 + row // 4
    kept = jnp.where(block < live_blocks[0, 0], expert_new, 0.0).astype(jnp.bfloat16)
    rank = lax.broadcasted_iota(jnp.int32, (8, 224, 128), 0)
    slices = jnp.where(rank_at(rank) == writer[0, 0, 0], kept[None], jnp.bfloat16(ABSENT))

    second = jnp.concatenate([slices, pair], axis=1)
    both = lax.all_to_all(
        second, EDP, split_axis=0, concat_axis=0, tiled=True, axis_index_groups=[RANKS]
    )
    partial = both[:, 224:].astype(jnp.float32).sum(axis=0)

    rows = partial.reshape(4, 7, 8, 128).transpose(0, 2, 1, 3).reshape(32, 7, 128)
    rows = jnp.concatenate([rows[FIRST:], rows[:FIRST]], axis=0)
    last = lax.all_to_all(
        rows, "zy", split_axis=0, concat_axis=0, tiled=True, axis_index_groups=[MEMBERS]
    )
    dense_sum = last.sum(axis=0).reshape(-1)

    state, expert_sum, both, _ = lax.optimization_barrier((state, expert_sum, both, rows))
    received = both[:, :224]
    expert_new, expert_mom, expert_sec = adam_update(*state, expert_sum)
    expert_new, expert_mom, expert_sec = (
        from_tiles(expert_new),
        from_tiles(expert_mom),
        from_tiles(expert_sec),
    )

    present = (received[:, 0, 0].astype(jnp.float32) < ABSENT / 2)
    index = rank_at(lax.broadcasted_iota(jnp.int32, (8, 8), 0))
    index2 = rank_at(lax.broadcasted_iota(jnp.int32, (8, 8), 1))
    before = jnp.sum(jnp.where((index2 < index) & present[None, :], 1, 0), axis=1)
    slot = lax.broadcasted_iota(jnp.int32, (4, 8), 0)
    selector = ((slot == before[None, :]) & present[None, :]).astype(jnp.bfloat16)
    clean = jnp.where(present[:, None, None], received, jnp.bfloat16(0))
    saved = jnp.einsum("kr,rql->kql", selector, clean, preferred_element_type=jnp.float32)
    saved = saved.astype(jnp.bfloat16).reshape(4, 56, 4, 128)
    saved = saved.transpose(0, 2, 1, 3).reshape(4, 28672)

    dense_new, dense_mom, dense_sec = adam_update(
        dense_param, dense_moment, dense_second, dense_sum
    )
    return (
        expert_new[None],
        expert_mom[None],
        expert_sec[None],
        dense_new,
        dense_mom,
        dense_sec,
        saved[None, None],
    )


def solution(mesh):
    fine = Mesh(mesh.devices.reshape(32, 2, 8), EP + (EDP,))
    state = P(EP, EDP, None)
    flat = P(EP + (EDP,))
    return jax.shard_map(
        body,
        mesh=fine,
        in_specs=(
            P(EP, EDP, None, None),
            state,
            state,
            state,
            P(EP, EDP, None, None),
            flat,
            flat,
            flat,
            state,
            P(EP, EDP),
        ),
        out_specs=(state, state, state, flat, flat, flat, P(EP, EDP, None, None)),
        check_vma=False,
    )
```

```python
import jax
import jax.numpy as jnp
from jax import lax
from jax.experimental import pallas as pl
from jax.sharding import Mesh, PartitionSpec as P


BETA_FIRST = 0.9
BETA_SECOND = 0.95
LEARN_RATE = 0.01
DECAY_RATE = 0.1
EPSILON = 1e-08
FIRST_BIAS = 1.0 - BETA_FIRST**10
SECOND_BIAS = 1.0 - BETA_SECOND**10
EP = ("zy", "c")
EDP = "r"
FIRST = 26
MEMBERS = [(FIRST + j) % 32 for j in range(32)]
LEAD = 3
RANKS = [j % 2 * 4 + (LEAD + j // 2) % 4 for j in range(8)]
ABSENT = 2.0**100


def adam_update(master, moment, second, gradient):
    moment_new = BETA_FIRST * moment + (1.0 - BETA_FIRST) * gradient
    second_new = BETA_SECOND * second + (1.0 - BETA_SECOND) * gradient * gradient
    direction = moment_new / FIRST_BIAS / (jnp.sqrt(second_new / SECOND_BIAS) + EPSILON)
    master_new = master - LEARN_RATE * (direction + DECAY_RATE * master)
    return (master_new, moment_new, second_new)


def to_tiles(x):
    return x.reshape(4, 56, 128).transpose(1, 0, 2).reshape(224, 128)


def from_tiles(x):
    return x.reshape(56, 4, 128).transpose(1, 0, 2).reshape(4, 7168)


def rank_at(place):
    return place % 2 * 4 + (LEAD + place // 2) % 4


def chunk_kernel(rows_ref, chunks_ref):
    for place, rank in enumerate(RANKS):
        chunks_ref[place] = rows_ref[4 * rank : 4 * rank + 4, :]


def body(
    expert_grads,
    expert_param,
    expert_moment,
    expert_second,
    dense_grads,
    dense_param,
    dense_moment,
    dense_second,
    writer,
    live_blocks,
):
    outgoing = pl.pallas_call(
        chunk_kernel,
        grid=(2,),
        in_specs=[pl.BlockSpec((32, 3584), lambda half: (0, half))],
        out_specs=pl.BlockSpec((8, 4, 3584), lambda half: (0, 0, half)),
        out_shape=jax.ShapeDtypeStruct((8, 4, 7168), jnp.bfloat16),
        name="chunks",
    )(expert_grads[0, 0])
    arrived = lax.all_to_all(
        outgoing, EDP, split_axis=0, concat_axis=0, tiled=True, axis_index_groups=[RANKS]
    )
    expert_sum = to_tiles(arrived.astype(jnp.float32).sum(axis=0))
    state = (to_tiles(expert_param[0]), to_tiles(expert_moment[0]), to_tiles(expert_second[0]))

    core = lax.axis_index("c")
    out_row = lax.broadcasted_iota(jnp.int32, (64, 64), 0)
    in_row = lax.broadcasted_iota(jnp.int32, (64, 64), 1)
    wanted = 2 * (out_row % 32) + jnp.where(out_row < 32, core, 1 - core)
    parting = (in_row == wanted).astype(jnp.bfloat16)
    parted = jnp.dot(parting, dense_grads[0, 0], preferred_element_type=jnp.float32)
    parted = parted.astype(jnp.bfloat16)
    swapped = lax.ppermute(parted[32:], "c", [(0, 1), (1, 0)])
    pair = parted[:32].astype(jnp.float32) + swapped.astype(jnp.float32)
    pair = pair.astype(jnp.bfloat16).reshape(4, 8, 2, 4, 7, 128).transpose(3, 2, 0, 4, 1, 5)
    pair = pair.reshape(8, 224, 128)
    pair = jnp.concatenate([pair[2 * LEAD :], pair[: 2 * LEAD]], axis=0)

    expert_new, _, _ = adam_update(*state, expert_sum)
    row = lax.broadcasted_iota(jnp.int32, (224, 128), 0)
    block = (row % 4) * 56 + row // 4
    kept = jnp.where(block < live_blocks[0, 0], expert_new, 0.0).astype(jnp.bfloat16)
    rank = lax.broadcasted_iota(jnp.int32, (8, 224, 128), 0)
    slices = jnp.where(rank_at(rank) == writer[0, 0, 0], kept[None], jnp.bfloat16(ABSENT))

    second = jnp.concatenate([slices, pair], axis=1)
    both = lax.all_to_all(
        second, EDP, split_axis=0, concat_axis=0, tiled=True, axis_index_groups=[RANKS]
    )
    partial = both[:, 224:].astype(jnp.float32).sum(axis=0)

    rows = partial.reshape(4, 7, 8, 128).transpose(0, 2, 1, 3).reshape(32, 7, 128)
    rows = rows.astype(jnp.bfloat16)
    rows = jnp.concatenate([rows[FIRST:], rows[:FIRST]], axis=0)
    last = lax.all_to_all(
        rows, "zy", split_axis=0, concat_axis=0, tiled=True, axis_index_groups=[MEMBERS]
    )
    dense_sum = last.astype(jnp.float32).sum(axis=0).reshape(-1)

    state, expert_sum, both, _ = lax.optimization_barrier((state, expert_sum, both, rows))
    received = both[:, :224]
    expert_new, expert_mom, expert_sec = adam_update(*state, expert_sum)
    expert_new, expert_mom, expert_sec = (
        from_tiles(expert_new),
        from_tiles(expert_mom),
        from_tiles(expert_sec),
    )

    present = (received[:, 0, 0].astype(jnp.float32) < ABSENT / 2)
    index = rank_at(lax.broadcasted_iota(jnp.int32, (8, 8), 0))
    index2 = rank_at(lax.broadcasted_iota(jnp.int32, (8, 8), 1))
    before = jnp.sum(jnp.where((index2 < index) & present[None, :], 1, 0), axis=1)
    slot = lax.broadcasted_iota(jnp.int32, (4, 8), 0)
    selector = ((slot == before[None, :]) & present[None, :]).astype(jnp.bfloat16)
    clean = jnp.where(present[:, None, None], received, jnp.bfloat16(0))
    saved = jnp.einsum("kr,rql->kql", selector, clean, preferred_element_type=jnp.float32)
    saved = saved.astype(jnp.bfloat16).reshape(4, 56, 4, 128)
    saved = saved.transpose(0, 2, 1, 3).reshape(4, 28672)

    dense_new, dense_mom, dense_sec = adam_update(
        dense_param, dense_moment, dense_second, dense_sum
    )
    return (
        expert_new[None],
        expert_mom[None],
        expert_sec[None],
        dense_new,
        dense_mom,
        dense_sec,
        saved[None, None],
    )


def solution(mesh):
    fine = Mesh(mesh.devices.reshape(32, 2, 8), EP + (EDP,))
    state = P(EP, EDP, None)
    flat = P(EP + (EDP,))
    return jax.shard_map(
        body,
        mesh=fine,
        in_specs=(
            P(EP, EDP, None, None),
            state,
            state,
            state,
            P(EP, EDP, None, None),
            flat,
            flat,
            flat,
            state,
            P(EP, EDP),
        ),
        out_specs=(state, state, state, flat, flat, flat, P(EP, EDP, None, None)),
        check_vma=False,
    )
```
